32 devices in a mesh: tok: 4 (over y, x), hid: 2 (over core), voc: 4 (over z).
Axes of the slice: x: 2, y: 2, z: 4, core: 2. Of those that a mesh axis runs over, the one named last changes fastest.
Arguments:
- student_hidden: bfloat16 [512, 8192], P('tok', ('hid', 'voc')), may hold values from -8 to 8
- teacher_hidden: bfloat16 [512, 16384], P('tok', ('hid', 'voc')), may hold values from -8 to 8
- student_head: bfloat16 [8192, 2048], P('hid', 'voc'), may hold values from -2 to 2
- teacher_head: bfloat16 [16384, 2048], P('hid', 'voc'), may hold values from -2 to 2
- loss_weight: float32 [512], P('tok'), may hold values from 128 to 1024
Outputs:
- grad_hidden: bfloat16 [512, 8192], P('tok', ('hid', 'voc'))
- mean_loss: float32 [], replicated
The draws below stay inside these ranges and needn't reach their ends.
All inputs are finite; a program needn't handle non-finite values.
Results may differ from the reference program's by a relative error of at most 0.001.
The reference program's roundings to bfloat16 on the way (of `scaled_gap`) count: a program that leaves them out, or rounds other values in their place, can miss the bound.
Values may be sent and summed in bfloat16 or wider, within the bound.
No kernel may reach another device: no remote copies, remote signals or barrier semaphores. Data moves between devices by JAX's collectives and lax.ppermute only.
A program may use at most 64 MiB of HBM per device.

```python
import math
import jax
import jax.numpy as jnp

DS = 8192
DT = 16384
TOKENS = 512
V = 2048


def head_values(key, width, salt):
    values = jax.random.normal(jax.random.fold_in(key, salt), (width, V), jnp.float32)
    return jnp.clip(values, -5.0, 5.0) * (2.0 / math.sqrt(width))


def hidden_values(key, width, head_salt, salt):
    values = jnp.clip(jax.random.normal(jax.random.fold_in(key, salt), (TOKENS, width), jnp.float32), -6.0, 6.0)
    return values


def draw_student_head(key, part):
    return head_values(key, DS, 11).astype(jnp.bfloat16)


def draw_teacher_head(key, part):
    return head_values(key, DT, 12).astype(jnp.bfloat16)


def draw_student_hidden(key, part):
    return hidden_values(key, DS, 11, 13).astype(jnp.bfloat16)


def draw_teacher_hidden(key, part):
    return hidden_values(key, DT, 12, 14).astype(jnp.bfloat16)


def block_levels(stream_key, shape, pieces, least, high):
    level = 1.0
    for dim, blocks in pieces:
        steps = jax.random.uniform(jax.random.fold_in(jax.random.fold_in(stream_key, 6), dim), (blocks,), jnp.float32, least / len(pieces), high / len(pieces))
        level = level * jnp.repeat(jnp.exp(steps), shape[dim] // blocks).reshape((-1,) + (1,) * (len(shape) - 1 - dim))
    return level


def setup_inputs(seed: int = 0) -> dict:
    key_of = jax.random.split(jax.random.key(seed), 6)
    return {
        "student_hidden": draw_student_hidden(jax.random.fold_in(key_of[5], 71), 0),
        "teacher_hidden": draw_teacher_hidden(jax.random.fold_in(key_of[5], 71), 0),
        "student_head": draw_student_head(jax.random.fold_in(key_of[5], 71), 0),
        "teacher_head": draw_teacher_head(jax.random.fold_in(key_of[5], 71), 0),
        "loss_weight": jnp.clip(jnp.exp(math.log(1024.0) - 2.0794415 * jax.random.uniform(key_of[4], (TOKENS,), jnp.float32) ** block_levels(key_of[4], (TOKENS,), ((0, 4),), -0.2, 0.2)), 128.0, 1024.0),
    }


def reference(student_hidden, teacher_hidden, student_head, teacher_head, loss_weight):
    student_logits = jnp.dot(student_hidden, student_head, preferred_element_type=jnp.float32)
    teacher_logits = jnp.dot(teacher_hidden, teacher_head, preferred_element_type=jnp.float32)
    student_peak = jnp.max(student_logits, axis=1)
    teacher_peak = jnp.max(teacher_logits, axis=1)
    student_lse = student_peak + jnp.log(jnp.sum(jnp.exp(student_logits - student_peak[:, None]), axis=1))
    teacher_lse = teacher_peak + jnp.log(jnp.sum(jnp.exp(teacher_logits - teacher_peak[:, None]), axis=1))
    teacher_prob = jnp.exp(teacher_logits - teacher_lse[:, None])
    student_prob = jnp.exp(student_logits - student_lse[:, None])
    divergence = jnp.sum(teacher_prob * (teacher_logits - student_logits), axis=1) - teacher_lse + student_lse
    mean_loss = jnp.sum(divergence) / TOKENS
    scaled_gap = (loss_weight[:, None] * (student_prob - teacher_prob)).astype(jnp.bfloat16)
    grad_hidden = jax.lax.dot_general(scaled_gap, student_head, (((1,), (1,)), ((), ())), preferred_element_type=jnp.float32)
    return grad_hidden.astype(jnp.bfloat16), mean_loss
```

```python
import jax
import jax.numpy as jnp
from jax import lax
from jax.sharding import PartitionSpec as P


GROUPS = 1
F32 = jnp.float32


def rotations(value, axis):
    size = lax.axis_size(axis)
    parts = [value]
    for r in range(1, size):
        parts.append(lax.ppermute(value, axis, [(j, (j - r) % size) for j in range(size)]))
    stacked = jnp.stack(parts + parts)
    return lax.dynamic_slice_in_dim(stacked, size - lax.axis_index(axis), size)


def total_over(value, axis):
    size = lax.axis_size(axis)
    total = value
    for r in range(1, size):
        total = total + lax.ppermute(value, axis, [(j, (j + r) % size) for j in range(size)])
    return total


def rows_of(head, block, size):
    rows = head.shape[0] // size
    return lax.dynamic_slice_in_dim(head, block * rows, rows)


def relay_steps(own, axis):
    size = lax.axis_size(axis)
    me = lax.axis_index(axis)
    right = left = own
    for s in range(1, size):
        right = lax.ppermute(right, axis, [(j, j + 1) for j in range(s - 1, size - 1)])
        left = lax.ppermute(left, axis, [(j, j - 1) for j in range(1, size - s + 1)])
        if 2 * s >= size:
            from_left = me >= s
            yield [(jnp.where(from_left, right, left), jnp.where(from_left, me - s, jnp.minimum(me + s, size - 1)))]
        else:
            yield [(right, jnp.maximum(me - s, 0)), (left, jnp.minimum(me + s, size - 1))]


def product(block, head, owner, size):
    return jnp.dot(block, rows_of(head, owner, size), preferred_element_type=F32)


def group_logits(student, teacher, student_head, teacher_head):
    size = lax.axis_size("voc")
    me = lax.axis_index("voc")
    student_sum = product(student, student_head, me, size)
    teacher_sum = product(teacher, teacher_head, me, size)
    for student_new, teacher_new in zip(relay_steps(student, "voc"), relay_steps(teacher, "voc")):
        for block, owner in student_new:
            student_sum = student_sum + product(block, student_head, owner, size)
        for block, owner in teacher_new:
            teacher_sum = teacher_sum + product(block, teacher_head, owner, size)
    return total_over(student_sum, "hid"), total_over(teacher_sum, "hid")


def group_gap(student_logits, teacher_logits, weights):
    peak_s = jnp.max(student_logits, axis=1)
    peak_t = jnp.max(teacher_logits, axis=1)
    exp_s = jnp.exp(student_logits - peak_s[:, None])
    exp_t = jnp.exp(teacher_logits - peak_t[:, None])
    local = jnp.stack(
        [
            peak_s,
            peak_t,
            jnp.sum(exp_s, axis=1),
            jnp.sum(exp_t, axis=1),
            jnp.sum(exp_t * (teacher_logits - student_logits), axis=1),
        ]
    )
    every = rotations(local, "voc")
    top_s = jnp.max(every[:, 0], axis=0)
    top_t = jnp.max(every[:, 1], axis=0)
    shrink_t = jnp.exp(every[:, 1] - top_t)
    total_s = jnp.sum(every[:, 2] * jnp.exp(every[:, 0] - top_s), axis=0)
    total_t = jnp.sum(every[:, 3] * shrink_t, axis=0)
    cross = jnp.sum(every[:, 4] * shrink_t, axis=0)
    lse_s = top_s + jnp.log(total_s)
    lse_t = top_t + jnp.log(total_t)
    divergence = cross / total_t - lse_t + lse_s
    gap = jnp.exp(student_logits - lse_s[:, None]) - jnp.exp(teacher_logits - lse_t[:, None])
    return (weights[:, None] * gap).astype(jnp.bfloat16), divergence


def group_grad(gap, student_head, scale, unscale, wire):
    size = lax.axis_size("voc")
    me = lax.axis_index("voc")

    def chunk(owner):
        out = lax.dot_general(
            gap, rows_of(student_head, owner, size), (((1,), (1,)), ((), ())), preferred_element_type=F32
        )
        return out * scale

    right = left = None
    for k in range(size - 1, 0, -1):
        if 2 * k >= size:
            part_right = part_left = chunk(jnp.where(me + k < size, me + k, jnp.maximum(me - k, 0)))
        else:
            part_right = chunk(jnp.minimum(me + k, size - 1))
            part_left = chunk(jnp.maximum(me - k, 0))
        if right is not None:
            part_right = part_right + right
            part_left = part_left + left
        right = lax.ppermute(part_right.astype(wire), "voc", [(j, j + 1) for j in range(size - k)]).astype(F32)
        left = lax.ppermute(part_left.astype(wire), "voc", [(j, j - 1) for j in range(k, size)]).astype(F32)
    own = chunk(me)
    if right is not None:
        own = own + right + left
    return (own * unscale).astype(jnp.bfloat16)


def shards(student_hidden, teacher_hidden, student_head, teacher_head, loss_weight):
    tokens = loss_weight.shape[0]
    size = lax.axis_size("voc")
    wire = jnp.float16 if size <= 8 else F32
    head_peak = jnp.max(jnp.abs(student_head)).astype(F32)
    head_peak = jnp.max(rotations(jnp.broadcast_to(head_peak, (1, 128)), "voc"))
    step = tokens // GROUPS
    grads, divergences = [], []
    for g in range(GROUPS):
        rows = slice(g * step, (g + 1) * step)
        weights = loss_weight[rows]
        student_logits, teacher_logits = group_logits(
            student_hidden[rows], teacher_hidden[rows], student_head, teacher_head
        )
        gap, divergence = group_gap(student_logits, teacher_logits, weights)
        bound = jnp.maximum(weights * head_peak, 1e-30)[:, None]
        grads.append(group_grad(gap, student_head, 16384.0 / bound, bound / 16384.0, wire))
        divergences.append(divergence)
    loss = sum(jnp.sum(d) for d in divergences)
    losses = rotations(jnp.broadcast_to(loss, (1, 128)), "tok")
    mean_loss = jnp.sum(losses[:, 0, 0]) / (tokens * lax.axis_size("tok"))
    return (jnp.concatenate(grads, axis=0), mean_loss)


def solution(mesh):
    placed = (
        P("tok", ("hid", "voc")),
        P("tok", ("hid", "voc")),
        P("hid", "voc"),
        P("hid", "voc"),
        P("tok"),
    )
    return jax.shard_map(
        shards,
        mesh=mesh,
        in_specs=placed,
        out_specs=(P("tok", ("hid", "voc")), P()),
        check_vma=False,
    )
```

```python
import jax
import jax.numpy as jnp
from jax import lax
from jax.sharding import PartitionSpec as P


GROUPS = 1
F32 = jnp.float32


def exchange(value, axis):
    size = lax.axis_size(axis)
    return [value] + [lax.ppermute(value, axis, [(j, j ^ r) for j in range(size)]) for r in range(1, size)]


def fold(values, combine):
    while len(values) > 1:
        values = [combine(values[j], values[j + 1]) for j in range(0, len(values), 2)]
    return values[0]


def add(a, b):
    return a + b


def squash(value, wire):
    if wire == F32:
        return value
    return (value * jnp.abs(value)).astype(wire)


def expand(value, wire):
    if wire == F32:
        return value
    value = value.astype(F32)
    return jnp.sign(value) * jnp.sqrt(jnp.abs(value))


def total_over(value, axis):
    size = lax.axis_size(axis)
    total = value
    for r in range(1, size):
        total = total + lax.ppermute(value, axis, [(j, (j + r) % size) for j in range(size)])
    return total


def rows_of(head, block, size):
    rows = head.shape[0] // size
    return lax.dynamic_slice_in_dim(head, block * rows, rows)


def relay_steps(own, axis):
    size = lax.axis_size(axis)
    me = lax.axis_index(axis)
    right = left = own
    for s in range(1, size):
        right = lax.ppermute(right, axis, [(j, j + 1) for j in range(s - 1, size - 1)])
        left = lax.ppermute(left, axis, [(j, j - 1) for j in range(1, size - s + 1)])
        if 2 * s >= size:
            from_left = me >= s
            yield [(jnp.where(from_left, right, left), jnp.where(from_left, me - s, jnp.minimum(me + s, size - 1)))]
        else:
            yield [(right, jnp.maximum(me - s, 0)), (left, jnp.minimum(me + s, size - 1))]


def product(block, head, owner, size):
    return jnp.dot(block, rows_of(head, owner, size), preferred_element_type=F32)


def group_logits(student, teacher, student_head, teacher_head, head_peak):
    size = lax.axis_size("voc")
    me = lax.axis_index("voc")
    student_sum = product(student, student_head, me, size)
    teacher_sum = product(teacher, teacher_head, me, size)
    student_sum, head_peak = lax.optimization_barrier((student_sum, head_peak))
    for student_new, teacher_new in zip(relay_steps(student, "voc"), relay_steps(teacher, "voc")):
        for block, owner in student_new:
            student_sum = student_sum + product(block, student_head, owner, size)
        for block, owner in teacher_new:
            teacher_sum = teacher_sum + product(block, teacher_head, owner, size)
    return total_over(student_sum, "hid"), total_over(teacher_sum, "hid"), head_peak


def group_gap(student_logits, teacher_logits, weights, head_peak):
    peak_s = jnp.max(student_logits, axis=1)
    peak_t = jnp.max(teacher_logits, axis=1)
    exp_s = jnp.exp(student_logits - peak_s[:, None])
    exp_t = jnp.exp(teacher_logits - peak_t[:, None])
    local = jnp.stack(
        [
            peak_s,
            peak_t,
            jnp.sum(exp_s, axis=1),
            jnp.sum(exp_t, axis=1),
            jnp.sum(exp_t * (teacher_logits - student_logits), axis=1),
            jnp.broadcast_to(head_peak, peak_s.shape),
        ]
    )
    every = exchange(local, "voc")
    tops = fold(every, jnp.maximum)
    top_s, top_t, head_peak = tops[0], tops[1], tops[5]
    shrinks = [jnp.exp(part[1] - top_t) for part in every]
    total_s = fold([part[2] * jnp.exp(part[0] - top_s) for part in every], add)
    total_t = fold([part[3] * shrink for part, shrink in zip(every, shrinks)], add)
    cross = fold([part[4] * shrink for part, shrink in zip(every, shrinks)], add)
    lse_s = top_s + jnp.log(total_s)
    lse_t = top_t + jnp.log(total_t)
    divergence = cross / total_t - lse_t + lse_s
    gap = jnp.exp(student_logits - lse_s[:, None]) - jnp.exp(teacher_logits - lse_t[:, None])
    spread = jnp.sqrt(2.0 * jnp.maximum(divergence, 0.0) + 2e-5)
    bound = jnp.maximum(weights * head_peak * spread, 1e-30)
    return (weights[:, None] * gap).astype(jnp.bfloat16), divergence, bound


def group_grad(gap, student_head, scale, unscale, wire, loss):
    size = lax.axis_size("voc")
    me = lax.axis_index("voc")

    def chunk(owner):
        out = lax.dot_general(
            gap, rows_of(student_head, owner, size), (((1,), (1,)), ((), ())), preferred_element_type=F32
        )
        return out * scale

    own = lax.optimization_barrier(chunk(me))
    right = left = None
    for k in range(size - 1, 0, -1):
        if 2 * k >= size:
            part_right = part_left = chunk(jnp.where(me + k < size, me + k, jnp.maximum(me - k, 0)))
        else:
            part_right = chunk(jnp.minimum(me + k, size - 1))
            part_left = chunk(jnp.maximum(me - k, 0))
        if right is not None:
            part_right, part_left = lax.optimization_barrier((part_right, part_left))
            part_right = part_right + expand(right, wire)
            part_left = part_left + expand(left, wire)
        part_right = squash(part_right, wire)
        part_left = squash(part_left, wire)
        if k == 1:
            loss, part_right, part_left = lax.optimization_barrier((loss, part_right, part_left))
        right = lax.ppermute(part_right, "voc", [(j, j + 1) for j in range(size - k)])
        left = lax.ppermute(part_left, "voc", [(j, j - 1) for j in range(k, size)])
    if right is not None:
        own = own + (expand(right, wire) + expand(left, wire))
    return (own * unscale).astype(jnp.bfloat16), loss


def shards(student_hidden, teacher_hidden, student_head, teacher_head, loss_weight):
    tokens = loss_weight.shape[0]
    wire = jnp.float16 if lax.axis_size("voc") <= 8 else F32
    head_peak = jnp.max(jnp.abs(student_head)).astype(F32)
    step = tokens // GROUPS
    grads, losses = [], []
    for g in range(GROUPS):
        rows = slice(g * step, (g + 1) * step)
        weights = loss_weight[rows]
        student_logits, teacher_logits, head_peak = group_logits(
            student_hidden[rows], teacher_hidden[rows], student_head, teacher_head, head_peak
        )
        gap, divergence, bound = group_gap(student_logits, teacher_logits, weights, head_peak)
        losses.append(jnp.sum(divergence))
        total = fold(losses, add) if g == GROUPS - 1 else losses[g]
        grad, total = group_grad(gap, student_head, (240.0 / bound)[:, None], (bound / 240.0)[:, None], wire, total)
        grads.append(grad)
    total = fold(exchange(jnp.broadcast_to(total, (1, 128)), "tok"), add)
    mean_loss = total[0, 0] / (tokens * lax.axis_size("tok"))
    return (jnp.concatenate(grads, axis=0), mean_loss)


def solution(mesh):
    placed = (
        P("tok", ("hid", "voc")),
        P("tok", ("hid", "voc")),
        P("hid", "voc"),
        P("hid", "voc"),
        P("tok"),
    )
    return jax.shard_map(
        shards,
        mesh=mesh,
        in_specs=placed,
        out_specs=(P("tok", ("hid", "voc")), P()),
        check_vma=False,
    )
```

```python
import jax
import jax.numpy as jnp
from jax import lax
from jax.sharding import PartitionSpec as P


GROUPS = 1
F32 = jnp.float32


def exchange(value, axis):
    size = lax.axis_size(axis)
    return [value] + [lax.ppermute(value, axis, [(j, j ^ r) for j in range(size)]) for r in range(1, size)]


def fold(values, combine):
    while len(values) > 1:
        values = [combine(values[j], values[j + 1]) for j in range(0, len(values), 2)]
    return values[0]


def add(a, b):
    return a + b


def squash(value, wire):
    if wire == F32:
        return value
    return (value * jnp.abs(value)).astype(wire)


def expand(value, wire):
    if wire == F32:
        return value
    value = value.astype(F32)
    return jnp.sign(value) * jnp.sqrt(jnp.abs(value))


def total_over(value, axis):
    size = lax.axis_size(axis)
    total = value
    for r in range(1, size):
        total = total + lax.ppermute(value, axis, [(j, (j + r) % size) for j in range(size)])
    return total


def rows_of(head, block, size):
    rows = head.shape[0] // size
    return lax.dynamic_slice_in_dim(head, block * rows, rows)


def spread_blocks(own, axis):
    size = lax.axis_size(axis)
    blocks = {0: own}
    bit = size // 2
    while bit:
        for offset in list(blocks):
            blocks[offset | bit] = lax.ppermute(blocks[offset], axis, [(j, j ^ bit) for j in range(size)])
        bit //= 2
    return blocks


def product(block, head, owner, size):
    return jnp.dot(block, rows_of(head, owner, size), preferred_element_type=F32)


def group_logits(student, teacher, student_head, teacher_head, head_peak):
    size = lax.axis_size("voc")
    me = lax.axis_index("voc")
    student_blocks = spread_blocks(student, "voc")
    teacher_blocks = spread_blocks(teacher, "voc")
    student_sum = product(student, student_head, me, size)
    teacher_sum = product(teacher, teacher_head, me, size)
    student_sum, head_peak = lax.optimization_barrier((student_sum, head_peak))
    for offset in list(student_blocks)[1:]:
        student_sum = student_sum + product(student_blocks[offset], student_head, me ^ offset, size)
        teacher_sum = teacher_sum + product(teacher_blocks[offset], teacher_head, me ^ offset, size)
    return total_over(student_sum, "hid"), total_over(teacher_sum, "hid"), head_peak


def group_gap(student_logits, teacher_logits, weights, head_peak):
    peak_s = jnp.max(student_logits, axis=1)
    peak_t = jnp.max(teacher_logits, axis=1)
    exp_s = jnp.exp(student_logits - peak_s[:, None])
    exp_t = jnp.exp(teacher_logits - peak_t[:, None])
    local = jnp.stack(
        [
            peak_s,
            peak_t,
            jnp.sum(exp_s, axis=1),
            jnp.sum(exp_t, axis=1),
            jnp.sum(exp_t * (teacher_logits - student_logits), axis=1),
            jnp.broadcast_to(head_peak, peak_s.shape),
        ]
    )
    every = exchange(local, "voc")
    tops = fold(every, jnp.maximum)
    top_s, top_t, head_peak = tops[0], tops[1], tops[5]
    shrinks = [jnp.exp(part[1] - top_t) for part in every]
    total_s = fold([part[2] * jnp.exp(part[0] - top_s) for part in every], add)
    total_t = fold([part[3] * shrink for part, shrink in zip(every, shrinks)], add)
    cross = fold([part[4] * shrink for part, shrink in zip(every, shrinks)], add)
    lse_s = top_s + jnp.log(total_s)
    lse_t = top_t + jnp.log(total_t)
    divergence = cross / total_t - lse_t + lse_s
    gap = jnp.exp(student_logits - lse_s[:, None]) - jnp.exp(teacher_logits - lse_t[:, None])
    spread = jnp.sqrt(2.0 * jnp.maximum(divergence, 0.0) + 2e-5)
    bound = jnp.maximum(weights * head_peak * spread, 1e-30)
    return (weights[:, None] * gap).astype(jnp.bfloat16), divergence, bound


def group_grad(gap, student_head, scale, unscale, wire, loss):
    size = lax.axis_size("voc")
    me = lax.axis_index("voc")

    def chunk(owner):
        out = lax.dot_general(
            gap, rows_of(student_head, owner, size), (((1,), (1,)), ((), ())), preferred_element_type=F32
        )
        return out * scale

    sums = {}
    bit = 1
    while bit < size:
        away = [o for o in range(size - 1, 0, -1) if o % (2 * bit) == bit]
        arrived = {}
        for offset in away:
            part = squash(sums.pop(offset) if offset in sums else chunk(me ^ offset), wire)
            if 2 * bit == size:
                loss, part = lax.optimization_barrier((loss, part))
            arrived[offset ^ bit] = lax.ppermute(part, "voc", [(j, j ^ bit) for j in range(size)])
        for offset, value in arrived.items():
            if offset not in sums:
                sums[offset] = lax.optimization_barrier(chunk(me ^ offset))
            sums[offset] = sums[offset] + expand(value, wire)
        bit *= 2
    own = sums[0] if sums else chunk(me)
    return (own * unscale).astype(jnp.bfloat16), loss


def shards(student_hidden, teacher_hidden, student_head, teacher_head, loss_weight):
    tokens = loss_weight.shape[0]
    wire = jnp.float16 if lax.axis_size("voc") <= 8 else F32
    head_peak = jnp.max(jnp.abs(student_head)).astype(F32)
    step = tokens // GROUPS
    grads, losses = [], []
    for g in range(GROUPS):
        rows = slice(g * step, (g + 1) * step)
        weights = loss_weight[rows]
        student_logits, teacher_logits, head_peak = group_logits(
            student_hidden[rows], teacher_hidden[rows], student_head, teacher_head, head_peak
        )
        gap, divergence, bound = group_gap(student_logits, teacher_logits, weights, head_peak)
        losses.append(jnp.sum(divergence))
        total = fold(losses, add) if g == GROUPS - 1 else losses[g]
        grad, total = group_grad(gap, student_head, (240.0 / bound)[:, None], (bound / 240.0)[:, None], wire, total)
        grads.append(grad)
    total = fold(exchange(jnp.broadcast_to(total, (1, 128)), "tok"), add)
    mean_loss = total[0, 0] / (tokens * lax.axis_size("tok"))
    return (jnp.concatenate(grads, axis=0), mean_loss)


def solution(mesh):
    placed = (
        P("tok", ("hid", "voc")),
        P("tok", ("hid", "voc")),
        P("hid", "voc"),
        P("hid", "voc"),
        P("tok"),
    )
    return jax.shard_map(
        shards,
        mesh=mesh,
        in_specs=placed,
        out_specs=(P("tok", ("hid", "voc")), P()),
        check_vma=False,
    )
```
